32 devices in a mesh: node: 16 (over z, y, core), harm: 2 (over x).
Axes of the slice: x: 2, y: 2, z: 4, core: 2. Of those that a mesh axis runs over, the one named last changes fastest.
Arguments:
- spectrum: float32 [128, 3, 98304], P('harm', None, 'node'), may hold values from -2 to 2
- source: float32 [128, 3, 98304], P('harm', None, 'node'), may hold values from -4 to 4
- coupling: bfloat16 [768, 4, 128, 128], P('node'), may hold values from -0.75 to 0.75
- capacitance: float32 [98304], P('node'), may hold values from 0.5 to 4
- saturation: float32 [98304], P('node'), may hold values from 0.1 to 1
- steepness: float32 [98304], P('node'), may hold values from 0.5 to 4
- junction: float32 [98304], P('node'), may hold values from 0.2 to 2
- halo_list: int32 [16, 4, 4], replicated, may hold values from 0 to 47, as said below
- neighbour_slot: int32 [768, 4], P('node'), may hold values from 0 to 64, as said below
Outputs:
- residual: float32 [128, 3, 98304], P('harm', None, 'node')
The draws below stay inside these ranges and needn't reach their ends.
Inputs may be any that keep to these rules, and one draw needn't show every extreme that they name: `halo_list`: row [m, j] lists 4 distinct blocks of device m, by index among its 48 blocks, needed by the device at index m + o_j along node, o = (-2, -1, 1, 2). `neighbour_slot`: column 0 of block b is b's own index among the 48 blocks of its device d. Other entries v: own block v if v < 48; block halo_list[m, j, s] of device m = d - o_j if v = 48 + j * 4 + s, only where m lies on the mesh; v = 64 is an empty entry. Every such slot of a device whose sender lies on the mesh is named by some entry of the device.
All inputs are finite; a program needn't handle non-finite values.
Results may differ from the reference program's by a relative error of at most 0.0025.
Values may be sent and summed in bfloat16 or wider, within the bound.
A program may use at most 128 MiB of HBM per device.

```python
import math
import jax
import jax.numpy as jnp
from jax import lax

HARMS = 64
SPEC = 128
BLK = 128
NNZ = 4
SLOTS = 4
POINTS = 3
NB_DEV = 48
NBLK = 768
NODES = 98304
N_NODE = 16


def draw_halo_list(key, part):
    keys = jax.random.split(key, N_NODE * 4)
    chosen = jax.vmap(lambda single: jax.random.permutation(single, NB_DEV)[:SLOTS])(keys)
    return chosen.reshape(N_NODE, 4, SLOTS).astype(jnp.int32)


def draw_neighbour_slot(key, part):
    empty_slot = NB_DEV + 4 * SLOTS
    entries = NB_DEV * (NNZ - 1)

    def per_device(device_key, device):
        first_key, second_key = jax.random.split(device_key)
        halo_slots = NB_DEV + jnp.arange(4 * SLOTS, dtype=jnp.int32)
        others = jax.random.randint(first_key, (entries - 4 * SLOTS,), 0, empty_slot + 1, dtype=jnp.int32)
        mixed = jax.random.permutation(second_key, jnp.concatenate([halo_slots, others]))
        direction = jnp.clip((mixed - NB_DEV) // SLOTS, 0, 3)
        offset = direction - 2 + (direction >= 2).astype(jnp.int32)
        sender = device - offset
        remote = (mixed >= NB_DEV) & (mixed < empty_slot)
        broken = remote & ((sender < 0) | (sender >= N_NODE))
        mixed = jnp.where(broken, empty_slot, mixed)
        own_column = jnp.arange(NB_DEV, dtype=jnp.int32)[:, None]
        return jnp.concatenate([own_column, mixed.reshape(NB_DEV, NNZ - 1)], axis=1)
    device_keys = jax.random.split(key, N_NODE)
    table = jax.vmap(per_device)(device_keys, jnp.arange(N_NODE, dtype=jnp.int32))
    return table.reshape(N_NODE * NB_DEV, NNZ).astype(jnp.int32)


def shard_levels(own_key, dims, cuts, least, top_value):
    factor_of = 1.0
    for dim, blocks in cuts:
        steps = jax.random.uniform(jax.random.fold_in(jax.random.fold_in(own_key, 6), dim), (blocks,), jnp.float32, least / len(cuts), top_value / len(cuts))
        factor_of = factor_of * jnp.repeat(jnp.exp(steps), dims[dim] // blocks).reshape((-1,) + (1,) * (len(dims) - 1 - dim))
    return factor_of


def centred(key, extent, spread, reach, cuts=(), kind=jnp.bfloat16):
    values = jax.random.normal(key, extent, jnp.float32) * spread
    if len(cuts) > 0:
        values = shard_levels(key, extent, cuts, -0.22, 0.18) * values
    return jnp.clip(values, min=-reach, max=reach).astype(kind)


def setup_inputs(seed: int = 0) -> dict:
    key_list = jax.random.split(jax.random.key(seed), 10)
    return {
        "spectrum": centred(key_list[0], (SPEC, POINTS, NODES), 0.15, 2.0, ((0, 2), (2, 16)), jnp.float32),
        "source": centred(key_list[1], (SPEC, POINTS, NODES), 0.3, 4.0, ((0, 2), (2, 16)), jnp.float32),
        "coupling": centred(key_list[2], (NBLK, NNZ, BLK, BLK), (NNZ * BLK // 8) ** -0.5, 0.75, ((0, 16),)),
        "capacitance": jnp.clip(jnp.exp(math.log(4.0) - 2.0794415 * jax.random.uniform(key_list[3], (NODES,), jnp.float32) ** shard_levels(key_list[3], (NODES,), ((0, 16),), -0.2, 0.2)), 0.5, 4.0),
        "saturation": jnp.clip(jnp.exp(math.log(1.0) - 2.3025851 * jax.random.uniform(key_list[4], (NODES,), jnp.float32) ** shard_levels(key_list[4], (NODES,), ((0, 16),), -0.2, 0.2)), 0.1, 1.0),
        "steepness": jnp.clip(jnp.exp(math.log(4.0) - 2.0794415 * jax.random.uniform(key_list[5], (NODES,), jnp.float32) ** shard_levels(key_list[5], (NODES,), ((0, 16),), -0.2, 0.2)), 0.5, 4.0),
        "junction": jnp.clip(jnp.exp(math.log(2.0) - 2.3025851 * jax.random.uniform(key_list[6], (NODES,), jnp.float32) ** shard_levels(key_list[6], (NODES,), ((0, 16),), -0.2, 0.2)), 0.2, 2.0),
        "halo_list": draw_halo_list(jax.random.fold_in(key_list[9], 71), 0),
        "neighbour_slot": draw_neighbour_slot(jax.random.fold_in(key_list[9], 71), 0),
    }


LOG_TWO = 0.6931471805599453

def synthesize(spectra):
    halfway = SPEC // 2
    cosines = spectra[0::2]
    sines = spectra[1::2]
    real_part = jnp.concatenate([cosines[:1] * SPEC, cosines[1:] * halfway, sines[:1] * SPEC], axis=0)
    zero_row = jnp.zeros_like(sines[:1])
    imag_part = jnp.concatenate([zero_row, -sines[1:] * halfway, zero_row], axis=0)
    return jnp.fft.irfft(real_part + 1j * imag_part, n=SPEC, axis=0).astype(jnp.float32)

def analyze(samples):
    halfway = SPEC // 2
    spectra = jnp.fft.rfft(samples, axis=0)
    lowest = spectra[0].real / SPEC
    highest = spectra[halfway].real / SPEC
    cosines = jnp.concatenate([lowest[None], 2.0 * spectra[1:halfway].real / SPEC], axis=0)
    sines = jnp.concatenate([highest[None], -2.0 * spectra[1:halfway].imag / SPEC], axis=0)
    return jnp.stack([cosines, sines], axis=1).reshape(SPEC, samples.shape[1]).astype(jnp.float32)

def derivative(spectra):
    pulsation = jnp.arange(SPEC // 2, dtype=jnp.float32)[:, None] / HARMS
    cosines = spectra[0::2]
    sines = spectra[1::2]
    return jnp.stack([pulsation * sines, -pulsation * cosines], axis=1).reshape(spectra.shape)

def single_level(spectrum, source, coupling, capacitance, saturation, steepness, junction, halo_list, neighbour_slot):
    rounded = spectrum.astype(jnp.bfloat16)
    blocks = rounded.reshape(SPEC, NBLK, BLK).transpose(1, 0, 2)
    offsets = jnp.array([-2, -1, 1, 2], dtype=jnp.int32)
    empty_slot = NB_DEV + 4 * SLOTS

    def per_device(device):
        slots = lax.dynamic_slice_in_dim(neighbour_slot, device * NB_DEV, NB_DEV, 0)
        relative = jnp.clip(slots - NB_DEV, 0, 4 * SLOTS - 1)
        direction = relative // SLOTS
        position = relative % SLOTS
        sender = jnp.clip(device - offsets[direction], 0, N_NODE - 1)
        remote = sender * NB_DEV + halo_list[sender, direction, position]
        global_id = jnp.where(slots < NB_DEV, device * NB_DEV + slots, remote)
        global_id = jnp.where(slots == empty_slot, 0, global_id).astype(jnp.int32)
        keep = (slots != empty_slot).astype(jnp.float32)
        picked = blocks[global_id].astype(jnp.float32) * keep[:, :, None, None]
        matrices = lax.dynamic_slice_in_dim(coupling, device * NB_DEV, NB_DEV, 0).astype(jnp.float32)
        return jnp.einsum('bksj,bkij->bsi', picked, matrices, precision=lax.Precision.HIGHEST)
    coupled = lax.map(per_device, jnp.arange(N_NODE, dtype=jnp.int32))
    coupled = coupled.reshape(NBLK, SPEC, BLK).transpose(1, 0, 2).reshape(SPEC, NODES)
    voltage = synthesize(spectrum)
    current = saturation * (jax.nn.softplus(steepness * voltage) - LOG_TWO)
    charge = junction * voltage / jnp.sqrt(1.0 + voltage * voltage)
    current_spec = analyze(current)
    charge_spec = analyze(charge)
    return coupled + derivative(capacitance * spectrum) + current_spec + derivative(charge_spec) - source

def reference(spectrum, source, coupling, capacitance, saturation, steepness, junction, halo_list, neighbour_slot):
    levels = []
    for level in range(POINTS):
        levels.append(single_level(spectrum[:, level], source[:, level], coupling, capacitance, saturation, steepness, junction, halo_list, neighbour_slot))
    return jnp.stack(levels, axis=1)
```

```python
import functools

import jax
import jax.numpy as jnp
import numpy as np
from jax import lax
from jax.experimental import pallas as pl
from jax.experimental.pallas import tpu as pltpu
from jax.sharding import PartitionSpec as P

LOG_TWO = 0.6931471805599453
OFFSETS = (-2, -1, 1, 2)
LANES = 128
CHUNK_BLOCKS = 8


def fourier_tables(length):
    sample = np.arange(length)[:, None]
    column = np.arange(length)[None, :]
    angle = 2.0 * np.pi / length * (column // 2 * sample % length)
    table = np.where(column % 2 == 1, np.sin(angle), np.cos(angle))
    table = np.where(column == 1, np.where(sample % 2 == 0, 1.0, -1.0), table)
    weights = np.where(np.arange(length) < 2, 1.0, 2.0) / length
    analysis = table.T * weights[:, None]
    pulsation = np.arange(length // 2)[:, None, None] / (length // 2)
    pairs = analysis.reshape(length // 2, 2, length)
    slope = np.concatenate([pulsation * pairs[:, 1:], -pulsation * pairs[:, :1]], axis=1)
    return table, analysis, slope.reshape(length, length)


def split(table):
    high = table.astype(jnp.bfloat16)
    low = (table - high.astype(jnp.float32)).astype(jnp.bfloat16)
    return high, low


def halo_kernel(list_ref, x_ref, *out_refs):
    slots = list_ref.shape[0] // len(out_refs)
    for direction, out_ref in enumerate(out_refs):
        for slot in range(slots):
            start = pl.multiple_of(list_ref[direction * slots + slot] * LANES, LANES)
            out_ref[:, :, slot * LANES : (slot + 1) * LANES] = x_ref[
                :, :, pl.ds(start, LANES)
            ].astype(jnp.bfloat16)


def coupling_kernel(per_step, slot_ref, x_ref, *refs):
    halo_refs = refs[: len(OFFSETS)]
    coupling_ref, source_ref, capacitance_ref, pulsation_ref, out_ref, pool_ref = refs[len(OFFSETS) :]
    points, rows, nodes = x_ref.shape
    own = nodes // LANES
    count = coupling_ref.shape[1]
    step = pl.program_id(0)

    @pl.when(step == 0)
    def _():
        for block in range(own):
            part = x_ref[:, :, block * LANES : (block + 1) * LANES].astype(jnp.bfloat16)
            pool_ref[block] = part.reshape(points * rows, LANES)
        place = own
        for halo_ref in halo_refs:
            for slot in range(halo_ref.shape[2] // LANES):
                part = halo_ref[:, :, slot * LANES : (slot + 1) * LANES]
                pool_ref[place] = part.reshape(points * rows, LANES)
                place += 1
        pool_ref[place] = jnp.zeros((points * rows, LANES), jnp.bfloat16)

    pulsation = pulsation_ref[...]
    even = lax.broadcasted_iota(jnp.int32, (rows, LANES), 0) % 2 == 0
    for inner in range(per_step):
        block = step * per_step + inner
        picked = [pool_ref[slot_ref[block * count + k]] for k in range(count)]
        gathered = jnp.concatenate(picked, axis=1)
        matrix = jnp.concatenate([coupling_ref[inner, k] for k in range(count)], axis=1)
        coupled = lax.dot_general(
            gathered, matrix, (((1,), (1,)), ((), ())), preferred_element_type=jnp.float32
        )
        lanes = pl.ds(inner * LANES, LANES)
        columns = pl.ds(pl.multiple_of(block * LANES, LANES), LANES)
        scaled = pulsation * capacitance_ref[:, lanes]
        for point in range(points):
            values = x_ref[point, :, columns]
            other = jnp.where(
                even, pltpu.roll(values, rows - 1, 0), pltpu.roll(values, 1, 0)
            )
            out_ref[point, :, lanes] = (
                coupled[point * rows : (point + 1) * rows]
                + scaled * other
                - source_ref[point, :, lanes]
            )


def nonlinear_kernel(shares, synthesis_ref, analysis_ref, *refs):
    spectra = refs[:shares]
    saturation_ref, steepness_ref, junction_ref, partial_ref, out_ref = refs[shares:]
    saturation = saturation_ref[...]
    steepness = steepness_ref[...]
    junction = junction_ref[...]
    synthesis = synthesis_ref[...]
    analysis = analysis_ref[...]
    for point in range(out_ref.shape[0]):
        columns = [ref[point] for ref in spectra]
        stacked = jnp.concatenate(columns + columns, axis=0)
        voltage = jnp.dot(synthesis, stacked, preferred_element_type=jnp.float32)
        drive = steepness * voltage
        softplus = jnp.maximum(drive, 0.0) + jnp.log(1.0 + jnp.exp(-jnp.abs(drive)))
        current = (saturation * (softplus - LOG_TWO)).astype(jnp.bfloat16)
        charge = (junction * voltage * lax.rsqrt(1.0 + voltage * voltage)).astype(jnp.bfloat16)
        samples = jnp.concatenate([current, charge], axis=0)
        out_ref[point] = partial_ref[point] + jnp.dot(
            analysis, samples, preferred_element_type=jnp.float32
        )


def local(
    spectrum,
    source,
    coupling,
    capacitance,
    saturation,
    steepness,
    junction,
    halo_list,
    neighbour_slot,
):
    rows, points, nodes = spectrum.shape
    shares = lax.axis_size("harm")
    length = rows * shares
    me = lax.axis_index("harm")
    whole = pl.BlockSpec(memory_space=pltpu.VMEM)
    x = jnp.transpose(spectrum, (1, 0, 2))
    injected = jnp.transpose(source, (1, 0, 2))

    blocks = nodes // LANES
    chunk_blocks = CHUNK_BLOCKS if blocks % CHUNK_BLOCKS == 0 else blocks
    width = chunk_blocks * LANES
    chunk_count = blocks // chunk_blocks
    own_chunks, arrived = [], []
    for chunk in range(chunk_count):
        piece = x[:, :, chunk * width : (chunk + 1) * width].astype(jnp.bfloat16)
        own_chunks.append(piece)
        arrived.append(
            [
                lax.ppermute(piece, "harm", [(i, (i + by) % shares) for i in range(shares)])
                for by in range(1, shares)
            ]
        )

    slots = halo_list.shape[2]
    listed = halo_list[lax.axis_index("node")].reshape(-1)
    packed = pl.pallas_call(
        halo_kernel,
        out_shape=[
            jax.ShapeDtypeStruct((points, rows, slots * LANES), jnp.bfloat16)
            for _ in OFFSETS
        ],
        in_specs=[pl.BlockSpec(memory_space=pltpu.SMEM), whole],
        out_specs=[whole for _ in OFFSETS],
        compiler_params=pltpu.CompilerParams(vmem_limit_bytes=16 << 20),
        cost_estimate=pl.CostEstimate(
            flops=0, bytes_accessed=points * rows * nodes * 4, transcendentals=0
        ),
        name="pack_halo",
    )(listed, x)
    devices = lax.axis_size("node")
    halos = [
        lax.ppermute(
            value, "node", [(i, i + by) for i in range(devices) if 0 <= i + by < devices]
        )
        for value, by in zip(packed, OFFSETS)
    ]

    count = neighbour_slot.shape[1]
    per_step = 4 if blocks % 4 == 0 else 1
    step_width = per_step * LANES
    row_ids = me * rows + jnp.arange(rows, dtype=jnp.int32)
    rate = (row_ids // 2).astype(jnp.float32) / (length // 2)
    rate = jnp.where(row_ids % 2 == 0, rate, -rate)
    rate = jnp.broadcast_to(rate[:, None], (rows, LANES))
    value_spec = pl.BlockSpec((points, rows, step_width), lambda i: (0, 0, i))
    partial = pl.pallas_call(
        functools.partial(coupling_kernel, per_step),
        grid=(blocks // per_step,),
        out_shape=jax.ShapeDtypeStruct((points, rows, nodes), jnp.float32),
        in_specs=[pl.BlockSpec(memory_space=pltpu.SMEM), whole]
        + [whole for _ in OFFSETS]
        + [
            pl.BlockSpec((per_step, count, LANES, LANES), lambda i: (i, 0, 0, 0)),
            value_spec,
            pl.BlockSpec((1, step_width), lambda i: (0, i)),
            whole,
        ],
        out_specs=value_spec,
        scratch_shapes=[
            pltpu.VMEM((blocks + len(OFFSETS) * slots + 1, points * rows, LANES), jnp.bfloat16)
        ],
        compiler_params=pltpu.CompilerParams(vmem_limit_bytes=32 << 20),
        cost_estimate=pl.CostEstimate(
            flops=2 * points * rows * nodes * count * LANES,
            bytes_accessed=coupling.size * 2 + 3 * x.size * 4,
            transcendentals=0,
        ),
        name="coupling",
    )(
        neighbour_slot.reshape(-1),
        x,
        *halos,
        coupling,
        injected,
        capacitance.reshape(1, -1),
        rate,
    )

    synthesis, analysis, slope = (
        jnp.asarray(table, jnp.float32) for table in fourier_tables(length)
    )
    senders = [(me - by) % shares for by in range(shares)]
    synthesis = jnp.concatenate(
        [lax.dynamic_slice_in_dim(synthesis, s * rows, rows, 1) for s in senders], axis=1
    )
    synthesis = jnp.concatenate(split(synthesis), axis=1)
    analysis = jnp.concatenate(
        [lax.dynamic_slice_in_dim(table, me * rows, rows, 0) for table in (analysis, slope)],
        axis=1,
    ).astype(jnp.bfloat16)
    scales = [value.reshape(1, -1) for value in (saturation, steepness, junction)]
    tile = 256 if width % 256 == 0 else width
    tiles = width // tile
    total = partial
    for chunk in range(chunk_count):
        first = chunk * tiles
        spectra = [own_chunks[chunk]] + arrived[chunk]
        here = pl.BlockSpec((points, rows, tile), lambda i, first=first: (0, 0, first + i))
        scale = pl.BlockSpec((1, tile), lambda i, first=first: (0, first + i))
        total = pl.pallas_call(
            functools.partial(nonlinear_kernel, shares),
            grid=(tiles,),
            out_shape=jax.ShapeDtypeStruct((points, rows, nodes), jnp.float32),
            in_specs=[whole, whole]
            + [pl.BlockSpec((points, rows, tile), lambda i: (0, 0, i)) for _ in spectra]
            + [scale] * 3
            + [here],
            out_specs=here,
            input_output_aliases={2 + shares + 3: 0},
            compiler_params=pltpu.CompilerParams(vmem_limit_bytes=32 << 20),
            cost_estimate=pl.CostEstimate(
                flops=8 * length * length * points * width,
                bytes_accessed=4 * points * rows * width * 3,
                transcendentals=3 * length * points * width,
            ),
            name="nonlinear",
        )(synthesis, analysis, *spectra, *scales, total)
    return jnp.transpose(total, (1, 0, 2))


def solution(mesh):
    in_specs = (
        P("harm", None, "node"),
        P("harm", None, "node"),
        P("node", None, None, None),
        P("node"),
        P("node"),
        P("node"),
        P("node"),
        P(),
        P("node", None),
    )
    out_specs = P("harm", None, "node")
    return jax.shard_map(local, mesh=mesh, in_specs=in_specs, out_specs=out_specs, check_vma=False)
```

```python
import functools

import jax
import jax.numpy as jnp
import numpy as np
from jax import lax
from jax.experimental import pallas as pl
from jax.experimental.pallas import tpu as pltpu
from jax.sharding import PartitionSpec as P

LOG_TWO = 0.6931471805599453
OFFSETS = (-2, -1, 1, 2)
LANES = 128
BOUNDS = (0, 4, 12, 20, 28, 36, 44, 48)
EARLY = 3
VMEM_BYTES = 60 << 20


def fourier_tables(length):
    sample = np.arange(length)[:, None]
    column = np.arange(length)[None, :]
    angle = 2.0 * np.pi / length * (column // 2 * sample % length)
    table = np.where(column % 2 == 1, np.sin(angle), np.cos(angle))
    table = np.where(column == 1, np.where(sample % 2 == 0, 1.0, -1.0), table)
    weights = np.where(np.arange(length) < 2, 1.0, 2.0) / length
    analysis = table.T * weights[:, None]
    pulsation = np.arange(length // 2)[:, None, None] / (length // 2)
    pairs = analysis.reshape(length // 2, 2, length)
    slope = np.concatenate([pulsation * pairs[:, 1:], -pulsation * pairs[:, :1]], axis=1)
    return table, analysis, slope.reshape(length, length)


def split(table):
    high = table.astype(jnp.bfloat16)
    low = (table - high.astype(jnp.float32)).astype(jnp.bfloat16)
    return high, low


def round_kernel(x_ref, out_ref):
    out_ref[...] = x_ref[...].astype(jnp.bfloat16)


def halo_kernel(list_ref, x_ref, *out_refs):
    slots = list_ref.shape[0] // len(out_refs)
    for direction, out_ref in enumerate(out_refs):
        for slot in range(slots):
            start = pl.multiple_of(list_ref[direction * slots + slot] * LANES, LANES)
            out_ref[:, :, slot * LANES : (slot + 1) * LANES] = x_ref[
                :, :, pl.ds(start, LANES)
            ].astype(jnp.bfloat16)


def coupling_kernel(per_step, early_steps, slot_ref, x_ref, *refs):
    halo_refs = refs[: len(OFFSETS)]
    coupling_ref, source_ref, capacitance_ref, pulsation_ref, before_ref, out_ref, pool_ref = refs[
        len(OFFSETS) :
    ]
    points, rows, nodes = x_ref.shape
    own = nodes // LANES
    count = coupling_ref.shape[1]
    step = pl.program_id(0)

    @pl.when(step == 0)
    def _():
        for block in range(own):
            part = x_ref[:, :, block * LANES : (block + 1) * LANES].astype(jnp.bfloat16)
            pool_ref[block] = part.reshape(points * rows, LANES)
        place = own
        for halo_ref in halo_refs:
            for slot in range(halo_ref.shape[2] // LANES):
                part = halo_ref[:, :, slot * LANES : (slot + 1) * LANES]
                pool_ref[place] = part.reshape(points * rows, LANES)
                place += 1
        pool_ref[place] = jnp.zeros((points * rows, LANES), jnp.bfloat16)

    pulsation = pulsation_ref[...]
    even = lax.broadcasted_iota(jnp.int32, (rows, LANES), 0) % 2 == 0
    for inner in range(per_step):
        block = step * per_step + inner
        picked = [pool_ref[slot_ref[block * count + k]] for k in range(count)]
        gathered = jnp.concatenate(picked, axis=1)
        matrix = jnp.concatenate([coupling_ref[inner, k] for k in range(count)], axis=1)
        coupled = lax.dot_general(
            gathered, matrix, (((1,), (1,)), ((), ())), preferred_element_type=jnp.float32
        )
        lanes = pl.ds(inner * LANES, LANES)
        columns = pl.ds(pl.multiple_of(block * LANES, LANES), LANES)
        scaled = pulsation * capacitance_ref[:, lanes]
        for point in range(points):
            values = x_ref[point, :, columns]
            other = jnp.where(
                even, pltpu.roll(values, rows - 1, 0), pltpu.roll(values, 1, 0)
            )
            before = jnp.where(step < early_steps, before_ref[point, :, lanes], 0.0)
            out_ref[point, :, lanes] = (
                before
                + coupled[point * rows : (point + 1) * rows]
                + scaled * other
                - source_ref[point, :, lanes]
            )


def nonlinear_kernel(shares, adds, synthesis_ref, analysis_ref, *refs):
    spectra = refs[:shares]
    saturation_ref, steepness_ref, junction_ref, *partial_ref, out_ref = refs[shares:]
    saturation = saturation_ref[...]
    steepness = steepness_ref[...]
    junction = junction_ref[...]
    synthesis = synthesis_ref[...]
    analysis = analysis_ref[...]
    for point in range(out_ref.shape[0]):
        columns = [ref[point] for ref in spectra]
        stacked = jnp.concatenate(columns + columns, axis=0)
        voltage = jnp.dot(synthesis, stacked, preferred_element_type=jnp.float32)
        drive = steepness * voltage
        softplus = jnp.maximum(drive, 0.0) + jnp.log(1.0 + jnp.exp(-jnp.abs(drive)))
        current = (saturation * (softplus - LOG_TWO)).astype(jnp.bfloat16)
        charge = (junction * voltage * lax.rsqrt(1.0 + voltage * voltage)).astype(jnp.bfloat16)
        samples = jnp.concatenate([current, charge], axis=0)
        result = jnp.dot(analysis, samples, preferred_element_type=jnp.float32)
        out_ref[point] = result + partial_ref[0][point] if adds else result


def call(kernel, grid, in_specs, out_specs, out_shape, flops, moved, **rest):
    return pl.pallas_call(
        kernel,
        grid=grid,
        in_specs=in_specs,
        out_specs=out_specs,
        out_shape=out_shape,
        compiler_params=pltpu.CompilerParams(vmem_limit_bytes=VMEM_BYTES),
        cost_estimate=pl.CostEstimate(flops=flops, bytes_accessed=moved, transcendentals=0),
        **rest,
    )


def local(
    spectrum,
    source,
    coupling,
    capacitance,
    saturation,
    steepness,
    junction,
    halo_list,
    neighbour_slot,
):
    rows, points, nodes = spectrum.shape
    shares = lax.axis_size("harm")
    length = rows * shares
    me = lax.axis_index("harm")
    x = jnp.transpose(spectrum, (1, 0, 2))
    injected = jnp.transpose(source, (1, 0, 2))
    smem = pl.BlockSpec(memory_space=pltpu.SMEM)

    def fixed(*shape):
        return pl.BlockSpec(shape, lambda i: (0,) * len(shape))

    blocks = nodes // LANES
    bounds = [bound * blocks // BOUNDS[-1] for bound in BOUNDS]
    unit = 2 if all(bound % 2 == 0 for bound in bounds) else 1
    tile = unit * LANES
    chunk_count = len(bounds) - 1
    own_chunks, arrived = [], []
    for chunk in range(chunk_count):
        low, high = bounds[chunk] * LANES, bounds[chunk + 1] * LANES
        if chunk == 0:
            shape = (points, rows, high)
            piece = call(
                round_kernel,
                (1,),
                [fixed(*shape)],
                fixed(*shape),
                jax.ShapeDtypeStruct(shape, jnp.bfloat16),
                0,
                points * rows * high * 6,
            )(x)
        else:
            piece = x[:, :, low:high].astype(jnp.bfloat16)
        own_chunks.append(piece)
        arrived.append(
            [
                lax.ppermute(piece, "harm", [(i, (i + by) % shares) for i in range(shares)])
                for by in range(1, shares)
            ]
        )

    slots = halo_list.shape[2]
    listed = halo_list[lax.axis_index("node")].reshape(-1)
    packed = call(
        halo_kernel,
        (1,),
        [smem, fixed(points, rows, nodes)],
        [fixed(points, rows, slots * LANES) for _ in OFFSETS],
        [jax.ShapeDtypeStruct((points, rows, slots * LANES), jnp.bfloat16) for _ in OFFSETS],
        0,
        points * rows * nodes * 4,
    )(listed, x)
    devices = lax.axis_size("node")
    halos = []
    for direction, by in enumerate(OFFSETS):
        pairs = [(i, i + by) for i in range(devices) if 0 <= i + by < devices]
        halos.append(lax.ppermute(packed[direction], "node", pairs))

    synthesis, analysis, slope = (
        jnp.asarray(table, jnp.float32) for table in fourier_tables(length)
    )
    senders = [(me - by) % shares for by in range(shares)]
    synthesis = jnp.concatenate(
        [lax.dynamic_slice_in_dim(synthesis, s * rows, rows, 1) for s in senders], axis=1
    )
    synthesis = jnp.concatenate(split(synthesis), axis=1)
    analysis = jnp.concatenate(
        [lax.dynamic_slice_in_dim(table, me * rows, rows, 0) for table in (analysis, slope)],
        axis=1,
    ).astype(jnp.bfloat16)
    scales = [value.reshape(1, -1) for value in (saturation, steepness, junction)]
    result_shape = jax.ShapeDtypeStruct((points, rows, nodes), jnp.float32)

    def nonlinear(chunk, total, adds):
        first = bounds[chunk] // unit
        width = (bounds[chunk + 1] - bounds[chunk]) * LANES
        spectra = [own_chunks[chunk]] + arrived[chunk]
        here = pl.BlockSpec((points, rows, tile), lambda i: (0, 0, first + i))
        before = [] if total is None else [total]
        before_spec = here if adds else pl.BlockSpec(memory_space=pl.ANY)
        return call(
            functools.partial(nonlinear_kernel, shares, adds),
            (width // tile,),
            [fixed(*synthesis.shape), fixed(*analysis.shape)]
            + [pl.BlockSpec((points, rows, tile), lambda i: (0, 0, i)) for _ in spectra]
            + [pl.BlockSpec((1, tile), lambda i: (0, first + i))] * 3
            + [before_spec for _ in before],
            here,
            result_shape,
            8 * length * length * points * width,
            4 * points * rows * width * 3,
            input_output_aliases={5 + shares: 0} if before else {},
        )(synthesis, analysis, *spectra, *scales, *before)

    total = None
    for chunk in range(EARLY):
        total = nonlinear(chunk, total, False)

    count = neighbour_slot.shape[1]
    per_step = 4 if all(bound % 4 == 0 for bound in bounds) else 1
    step_width = per_step * LANES
    row_ids = me * rows + jnp.arange(rows, dtype=jnp.int32)
    rate = (row_ids // 2).astype(jnp.float32) / (length // 2)
    rate = jnp.where(row_ids % 2 == 0, rate, -rate)
    rate = jnp.broadcast_to(rate[:, None], (rows, LANES))
    value_spec = pl.BlockSpec((points, rows, step_width), lambda i: (0, 0, i))
    total = call(
        functools.partial(coupling_kernel, per_step, bounds[EARLY] // per_step),
        (blocks // per_step,),
        [smem, fixed(points, rows, nodes)]
        + [fixed(points, rows, slots * LANES) for _ in OFFSETS]
        + [
            pl.BlockSpec((per_step, count, LANES, LANES), lambda i: (i, 0, 0, 0)),
            value_spec,
            pl.BlockSpec((1, step_width), lambda i: (0, i)),
            fixed(rows, LANES),
            value_spec,
        ],
        value_spec,
        result_shape,
        2 * points * rows * nodes * count * LANES,
        coupling.size * 2 + 3 * x.size * 4,
        scratch_shapes=[
            pltpu.VMEM((blocks + len(OFFSETS) * slots + 1, points * rows, LANES), jnp.bfloat16)
        ],
        input_output_aliases={6 + len(OFFSETS): 0},
    )(
        neighbour_slot.reshape(-1),
        x,
        *halos,
        coupling,
        injected,
        capacitance.reshape(1, -1),
        rate,
        total,
    )
    for chunk in range(EARLY, chunk_count):
        total = nonlinear(chunk, total, True)
    return jnp.transpose(total, (1, 0, 2))


def solution(mesh):
    in_specs = (
        P("harm", None, "node"),
        P("harm", None, "node"),
        P("node", None, None, None),
        P("node"),
        P("node"),
        P("node"),
        P("node"),
        P(),
        P("node", None),
    )
    out_specs = P("harm", None, "node")
    return jax.shard_map(local, mesh=mesh, in_specs=in_specs, out_specs=out_specs, check_vma=False)
```

```python
import functools

import jax
import jax.numpy as jnp
import numpy as np
from jax import lax
from jax.experimental import pallas as pl
from jax.experimental.pallas import tpu as pltpu
from jax.sharding import PartitionSpec as P

LOG_TWO = 0.6931471805599453
OFFSETS = (-2, -1, 1, 2)
LANES = 128
BOUNDS = (0, 8, 24, 40, 48)
EARLY = 2
VMEM_BYTES = 60 << 20


def fourier_tables(length):
    sample = np.arange(length)[:, None]
    column = np.arange(length)[None, :]
    angle = 2.0 * np.pi / length * (column // 2 * sample % length)
    table = np.where(column % 2 == 1, np.sin(angle), np.cos(angle))
    table = np.where(column == 1, np.where(sample % 2 == 0, 1.0, -1.0), table)
    weights = np.where(np.arange(length) < 2, 1.0, 2.0) / length
    analysis = table.T * weights[:, None]
    pulsation = np.arange(length // 2)[:, None, None] / (length // 2)
    pairs = analysis.reshape(length // 2, 2, length)
    slope = np.concatenate([pulsation * pairs[:, 1:], -pulsation * pairs[:, :1]], axis=1)
    return table, analysis, slope.reshape(length, length)


def split(table):
    high = table.astype(jnp.bfloat16)
    low = (table - high.astype(jnp.float32)).astype(jnp.bfloat16)
    return high, low


def round_kernel(x_ref, out_ref):
    out_ref[...] = x_ref[...].astype(jnp.bfloat16)


def halo_kernel(list_ref, x_ref, *out_refs):
    slots = list_ref.shape[0] // len(out_refs)
    for direction, out_ref in enumerate(out_refs):
        for slot in range(slots):
            start = pl.multiple_of(list_ref[direction * slots + slot] * LANES, LANES)
            out_ref[:, :, slot * LANES : (slot + 1) * LANES] = x_ref[
                :, :, pl.ds(start, LANES)
            ].astype(jnp.bfloat16)


def coupling_kernel(per_step, early_steps, slot_ref, x_ref, *refs):
    halo_refs = refs[: len(OFFSETS)]
    coupling_ref, source_ref, capacitance_ref, pulsation_ref, before_ref, out_ref, pool_ref = refs[
        len(OFFSETS) :
    ]
    points, rows, nodes = x_ref.shape
    own = nodes // LANES
    count = coupling_ref.shape[1]
    step = pl.program_id(0)

    @pl.when(step == 0)
    def _():
        for block in range(own):
            part = x_ref[:, :, block * LANES : (block + 1) * LANES].astype(jnp.bfloat16)
            pool_ref[block] = part.reshape(points * rows, LANES)
        place = own
        for halo_ref in halo_refs:
            for slot in range(halo_ref.shape[2] // LANES):
                part = halo_ref[:, :, slot * LANES : (slot + 1) * LANES]
                pool_ref[place] = part.reshape(points * rows, LANES)
                place += 1
        pool_ref[place] = jnp.zeros((points * rows, LANES), jnp.bfloat16)

    pulsation = pulsation_ref[...]
    even = lax.broadcasted_iota(jnp.int32, (rows, LANES), 0) % 2 == 0
    for inner in range(per_step):
        block = step * per_step + inner
        picked = [pool_ref[slot_ref[block * count + k]] for k in range(count)]
        gathered = jnp.concatenate(picked, axis=1)
        matrix = jnp.concatenate([coupling_ref[inner, k] for k in range(count)], axis=1)
        coupled = lax.dot_general(
            gathered, matrix, (((1,), (1,)), ((), ())), preferred_element_type=jnp.float32
        )
        lanes = pl.ds(inner * LANES, LANES)
        columns = pl.ds(pl.multiple_of(block * LANES, LANES), LANES)
        scaled = pulsation * capacitance_ref[:, lanes]
        for point in range(points):
            values = x_ref[point, :, columns]
            other = jnp.where(
                even, pltpu.roll(values, rows - 1, 0), pltpu.roll(values, 1, 0)
            )
            before = jnp.where(step < early_steps, before_ref[point, :, lanes], 0.0)
            out_ref[point, :, lanes] = (
                before
                + coupled[point * rows : (point + 1) * rows]
                + scaled * other
                - source_ref[point, :, lanes]
            )


def nonlinear_kernel(shares, adds, synthesis_ref, analysis_ref, *refs):
    spectra = refs[:shares]
    saturation_ref, steepness_ref, junction_ref, *partial_ref, out_ref = refs[shares:]
    saturation = saturation_ref[...]
    steepness = steepness_ref[...]
    junction = junction_ref[...]
    synthesis = synthesis_ref[...]
    analysis = analysis_ref[...]
    for point in range(out_ref.shape[0]):
        columns = [ref[point] for ref in spectra]
        stacked = jnp.concatenate(columns + columns, axis=0)
        voltage = jnp.dot(synthesis, stacked, preferred_element_type=jnp.float32)
        drive = steepness * voltage
        softplus = jnp.maximum(drive, 0.0) + jnp.log(1.0 + jnp.exp(-jnp.abs(drive)))
        current = (saturation * (softplus - LOG_TWO)).astype(jnp.bfloat16)
        charge = (junction * voltage * lax.rsqrt(1.0 + voltage * voltage)).astype(jnp.bfloat16)
        samples = jnp.concatenate([current, charge], axis=0)
        result = jnp.dot(analysis, samples, preferred_element_type=jnp.float32)
        out_ref[point] = result + partial_ref[0][point] if adds else result


def call(kernel, grid, in_specs, out_specs, out_shape, flops, moved, **rest):
    return pl.pallas_call(
        kernel,
        grid=grid,
        in_specs=in_specs,
        out_specs=out_specs,
        out_shape=out_shape,
        compiler_params=pltpu.CompilerParams(vmem_limit_bytes=VMEM_BYTES),
        cost_estimate=pl.CostEstimate(flops=flops, bytes_accessed=moved, transcendentals=0),
        **rest,
    )


def local(
    spectrum,
    source,
    coupling,
    capacitance,
    saturation,
    steepness,
    junction,
    halo_list,
    neighbour_slot,
):
    rows, points, nodes = spectrum.shape
    shares = lax.axis_size("harm")
    length = rows * shares
    me = lax.axis_index("harm")
    x = jnp.transpose(spectrum, (1, 0, 2))
    injected = jnp.transpose(source, (1, 0, 2))
    smem = pl.BlockSpec(memory_space=pltpu.SMEM)

    def fixed(*shape):
        return pl.BlockSpec(shape, lambda i: (0,) * len(shape))

    blocks = nodes // LANES
    bounds = [bound * blocks // BOUNDS[-1] for bound in BOUNDS]
    unit = 8 if all(bound % 8 == 0 for bound in bounds) else 1
    tile = unit * LANES
    chunk_count = len(bounds) - 1
    own_chunks, arrived = [], []
    for chunk in range(chunk_count):
        low, high = bounds[chunk] * LANES, bounds[chunk + 1] * LANES
        if chunk == 0:
            shape = (points, rows, high)
            piece = call(
                round_kernel,
                (1,),
                [fixed(*shape)],
                fixed(*shape),
                jax.ShapeDtypeStruct(shape, jnp.bfloat16),
                0,
                points * rows * high * 6,
            )(x)
        else:
            piece = x[:, :, low:high].astype(jnp.bfloat16)
        own_chunks.append(piece)
        arrived.append(
            [
                lax.ppermute(piece, "harm", [(i, (i + by) % shares) for i in range(shares)])
                for by in range(1, shares)
            ]
        )

    slots = halo_list.shape[2]
    listed = halo_list[lax.axis_index("node")].reshape(-1)
    packed = call(
        halo_kernel,
        (1,),
        [smem, fixed(points, rows, nodes)],
        [fixed(points, rows, slots * LANES) for _ in OFFSETS],
        [jax.ShapeDtypeStruct((points, rows, slots * LANES), jnp.bfloat16) for _ in OFFSETS],
        0,
        points * rows * nodes * 4,
    )(listed, x)
    devices = lax.axis_size("node")
    halos = []
    for direction, by in enumerate(OFFSETS):
        pairs = [(i, i + by) for i in range(devices) if 0 <= i + by < devices]
        halos.append(lax.ppermute(packed[direction], "node", pairs))

    synthesis, analysis, slope = (
        jnp.asarray(table, jnp.float32) for table in fourier_tables(length)
    )
    senders = [(me - by) % shares for by in range(shares)]
    synthesis = jnp.concatenate(
        [lax.dynamic_slice_in_dim(synthesis, s * rows, rows, 1) for s in senders], axis=1
    )
    synthesis = jnp.concatenate(split(synthesis), axis=1)
    analysis = jnp.concatenate(
        [lax.dynamic_slice_in_dim(table, me * rows, rows, 0) for table in (analysis, slope)],
        axis=1,
    ).astype(jnp.bfloat16)
    scales = [value.reshape(1, -1) for value in (saturation, steepness, junction)]
    result_shape = jax.ShapeDtypeStruct((points, rows, nodes), jnp.float32)

    def nonlinear(chunk, total, adds):
        first = bounds[chunk] // unit
        width = (bounds[chunk + 1] - bounds[chunk]) * LANES
        spectra = [own_chunks[chunk]] + arrived[chunk]
        here = pl.BlockSpec((points, rows, tile), lambda i: (0, 0, first + i))
        before = [] if total is None else [total]
        before_spec = here if adds else pl.BlockSpec(memory_space=pl.ANY)
        return call(
            functools.partial(nonlinear_kernel, shares, adds),
            (width // tile,),
            [fixed(*synthesis.shape), fixed(*analysis.shape)]
            + [pl.BlockSpec((points, rows, tile), lambda i: (0, 0, i)) for _ in spectra]
            + [pl.BlockSpec((1, tile), lambda i: (0, first + i))] * 3
            + [before_spec for _ in before],
            here,
            result_shape,
            8 * length * length * points * width,
            4 * points * rows * width * 3,
            input_output_aliases={5 + shares: 0} if before else {},
        )(synthesis, analysis, *spectra, *scales, *before)

    total = None
    for chunk in range(EARLY):
        total = nonlinear(chunk, total, False)

    count = neighbour_slot.shape[1]
    per_step = unit
    step_width = per_step * LANES
    row_ids = me * rows + jnp.arange(rows, dtype=jnp.int32)
    rate = (row_ids // 2).astype(jnp.float32) / (length // 2)
    rate = jnp.where(row_ids % 2 == 0, rate, -rate)
    rate = jnp.broadcast_to(rate[:, None], (rows, LANES))
    value_spec = pl.BlockSpec((points, rows, step_width), lambda i: (0, 0, i))
    total = call(
        functools.partial(coupling_kernel, per_step, bounds[EARLY] // per_step),
        (blocks // per_step,),
        [smem, fixed(points, rows, nodes)]
        + [fixed(points, rows, slots * LANES) for _ in OFFSETS]
        + [
            pl.BlockSpec((per_step, count, LANES, LANES), lambda i: (i, 0, 0, 0)),
            value_spec,
            pl.BlockSpec((1, step_width), lambda i: (0, i)),
            fixed(rows, LANES),
            value_spec,
        ],
        value_spec,
        result_shape,
        2 * points * rows * nodes * count * LANES,
        coupling.size * 2 + 3 * x.size * 4,
        scratch_shapes=[
            pltpu.VMEM((blocks + len(OFFSETS) * slots + 1, points * rows, LANES), jnp.bfloat16)
        ],
        input_output_aliases={6 + len(OFFSETS): 0},
    )(
        neighbour_slot.reshape(-1),
        x,
        *halos,
        coupling,
        injected,
        capacitance.reshape(1, -1),
        rate,
        total,
    )
    for chunk in range(EARLY, chunk_count):
        total = nonlinear(chunk, total, True)
    return jnp.transpose(total, (1, 0, 2))


def solution(mesh):
    in_specs = (
        P("harm", None, "node"),
        P("harm", None, "node"),
        P("node", None, None, None),
        P("node"),
        P("node"),
        P("node"),
        P("node"),
        P(),
        P("node", None),
    )
    out_specs = P("harm", None, "node")
    return jax.shard_map(local, mesh=mesh, in_specs=in_specs, out_specs=out_specs, check_vma=False)
```
